256 devices in a mesh: expert: 16 (over z, core), hidden: 16 (over x, y).
Axes of the slice: x: 4, y: 4, z: 8, core: 2. Of those that a mesh axis runs over, the one named last changes fastest.
Arguments:
- inputs: bfloat16 [3072, 2880], P('expert', 'hidden'), may hold values from -6 to 6
- out_grad: bfloat16 [3072, 2880], P('expert', 'hidden'), may hold values from -6 to 6
- expert_ids: int32 [3072, 4], P('expert'), may hold values from 0 to 15, all different within a row; in each aligned block of 192 rows (0 to 191, 192 to 383, ...) at most 72 rows name the same one
- route_weight: float32 [3072, 4], P('expert'), may hold values from 0.1 to 1
- w_gate: bfloat16 [16, 2880, 2880], P('expert', 'hidden'), may hold values from -0.109375 to 0.109375
- w_up: bfloat16 [16, 2880, 2880], P('expert', 'hidden'), may hold values from -0.109375 to 0.109375
- w_down: bfloat16 [16, 2880, 2880], P('expert', 'hidden'), may hold values from -0.109375 to 0.109375
Outputs:
- grad_input: bfloat16 [3072, 2880], P('expert', 'hidden')
- grad_route: float32 [3072, 4], P('expert')
- grad_gate: float32 [16, 2880, 2880], P('expert', 'hidden')
- grad_up: float32 [16, 2880, 2880], P('expert', 'hidden')
- grad_down: float32 [16, 2880, 2880], P('expert', 'hidden')
The draws below stay inside these ranges and needn't reach their ends.
Inputs may be any that keep to these rules, and one draw needn't show every extreme that they name: `expert_ids`: each token names 4 different experts. Among the 192 tokens of one index of the expert axis no expert is named more than 72 times, a bound that some block reaches.
All inputs are finite; a program needn't handle non-finite values.
Results may differ from the reference program's by a relative error of at most 0.018.
Values may be sent and summed in bfloat16 or wider, within the bound.
A program may use at most 128 MiB of HBM per device.

```python
import math
import jax
import jax.numpy as jnp
import numpy as np
from jax import lax

D = 2880
FF = 2880
TOP = 4
TOK_DEV = 192
EXPERTS = 16
TOKENS = 3072
CAP = 72
N_EXPERT = 16


def steps_of(rng, extent, split, least, high):
    def one(axis_at, parts):
        heights = jax.random.uniform(jax.random.fold_in(jax.random.fold_in(rng, 6), axis_at), (parts,), jnp.float32, least / len(split), high / len(split))
        return jnp.repeat(jnp.exp(heights), extent[axis_at] // parts).reshape((-1,) + (1,) * (len(extent) - axis_at - 1))

    loudness = one(*split[0])
    for cut in split[1:]:
        loudness = loudness * one(*cut)
    return loudness


def deal_out(stream_key, own, number, rows, amount, top, most, skew):
    sequence = jax.random.permutation(stream_key, amount)
    crowded, common = shares(amount, rows * top, most, skew, True), shares(amount, rows * top, most, skew, False)
    places = jnp.arange(amount)

    def named(tallies, rotation):
        used = int((tallies > 0).sum())
        fixed = max(1, used // 4)
        moved = fixed + (places - fixed + rotation * (used - fixed)) % max(1, amount - fixed)
        return jnp.zeros((amount,), jnp.int32).at[sequence[jnp.where(places < fixed, places, moved)]].set(jnp.asarray(tallies, jnp.int32))

    tallies = jnp.where(number % 4 == 0, named(crowded, number // 4), named(common, number - number // 4 - 1))
    mixed = jax.random.permutation(jax.random.fold_in(own, 3), amount)
    donor, sink = mixed[0:amount // 2 * 2:2], mixed[1:amount // 2 * 2:2]
    room = jnp.minimum(tallies[donor] - 1, most - tallies[sink]) // 2
    room = jnp.where((donor == sequence[0]) | (sink == sequence[0]) | (tallies[sink] == 0), 0, jnp.maximum(room, 0))
    moved = jax.random.randint(jax.random.fold_in(own, 4), (amount // 2,), 0, 1 << 20) % (room + 1)
    tallies = tallies.at[donor].add(-moved).at[sink].add(moved)
    members = jnp.searchsorted(jnp.cumsum(tallies), jnp.arange(rows * top), side="right").astype(jnp.int32)
    grid = members.reshape(top, rows).T
    grid = grid[jax.random.permutation(jax.random.fold_in(own, 1), rows)]
    rotation = jax.random.randint(jax.random.fold_in(own, 2), (rows, 1), 0, top)
    return jnp.take_along_axis(grid, (jnp.arange(top)[None, :] + rotation) % top, axis=1)


def shares(amount, total, limit, lean, full):
    weights = [(1 << 20) // math.isqrt(standing ** lean) + 1 for standing in range(1, amount + 1)]
    largest = limit if full else min(limit, max(-(-total // amount), total * weights[0] // sum(weights)))
    least = 1 if total - largest >= amount - 1 else 0
    holding, spare = [largest] + [least] * (amount - 1), total - largest - least * (amount - 1)
    while spare > 0:
        movable = [i for i in range(1, amount) if holding[i] < largest] or [i for i in range(1, amount) if holding[i] < limit]
        whole, remaining = sum([weights[i] for i in movable]), spare
        for i in movable:
            more = min(limit - holding[i], max(1, remaining * weights[i] // whole), spare)
            holding[i] = holding[i] + more
            spare = spare - more
    return np.array(holding)


def noise(stream_key, extent, deviation, limit, cuts=(), kind=jnp.bfloat16):
    loudness = steps_of(stream_key, extent, cuts, -0.22, 0.18) if cuts else 1.0
    array = jax.random.normal(stream_key, extent, jnp.float32) * deviation * loudness
    return jnp.minimum(jnp.maximum(array, -limit), limit).astype(kind)


def setup_inputs(seed: int = 0) -> dict:
    splits = jax.random.split(jax.random.key(seed), 8)
    inputs = noise(splits[0], (TOKENS, D), 1.0, 6.0, ((0, 16), (1, 16)))
    out_grad = noise(splits[1], (TOKENS, D), 1.0, 6.0, ((0, 16), (1, 16)))
    expert_ids_keys = jax.random.split(jax.random.fold_in(splits[2], 1), TOKENS // TOK_DEV)
    expert_ids_turns = jax.random.permutation(jax.random.fold_in(splits[2], 3), TOKENS // TOK_DEV)
    expert_ids = jax.vmap(lambda own, number: deal_out(jax.random.fold_in(splits[2], 2), own, number, TOK_DEV, EXPERTS, TOP, CAP, 2))(expert_ids_keys, expert_ids_turns).reshape((TOKENS, TOP))
    route_weight = jnp.clip(0.1 + 0.9 * jax.random.uniform(splits[3], (TOKENS, TOP), jnp.float32) ** steps_of(splits[3], (TOKENS, TOP), ((0, 16),), -0.2, 0.2), 0.1, 1.0)
    w_gate = noise(splits[4], (EXPERTS, FF, D), D ** -0.5, 0.109375, ((0, 16), (1, 16)))
    w_up = noise(splits[5], (EXPERTS, FF, D), D ** -0.5, 0.109375, ((0, 16), (1, 16)))
    w_down = noise(splits[6], (EXPERTS, FF, D), FF ** -0.5, 0.109375, ((0, 16), (1, 16)))
    return {"inputs": inputs, "out_grad": out_grad, "expert_ids": expert_ids, "route_weight": route_weight, "w_gate": w_gate, "w_up": w_up, "w_down": w_down}


def reference(inputs, out_grad, expert_ids, route_weight, w_gate, w_up, w_down):
    pairs = TOK_DEV * TOP
    ids = expert_ids.reshape(N_EXPERT, pairs).astype(jnp.int32)
    onehot = (ids[:, :, None] == jnp.arange(EXPERTS, dtype=jnp.int32)[None, None, :]).astype(jnp.int32)
    position = jnp.cumsum(onehot, axis=1) - 1
    slot = jnp.sum(onehot * position, axis=2).astype(jnp.int32)
    source = jnp.arange(N_EXPERT, dtype=jnp.int32)[:, None]
    where = (ids * (N_EXPERT * CAP) + source * CAP + slot).reshape(-1).astype(jnp.int32)
    assign = jnp.arange(N_EXPERT * pairs, dtype=jnp.int32)
    table = jnp.zeros((EXPERTS * N_EXPERT * CAP,), jnp.int32).at[where].set(assign)
    filled = jnp.zeros((EXPERTS * N_EXPERT * CAP,), jnp.int32).at[where].set(1)
    table = table.reshape(EXPERTS, N_EXPERT * CAP)
    filled = filled.reshape(EXPERTS, N_EXPERT * CAP)
    flat_weight = route_weight.reshape(-1)

    def one_expert(carry, pieces):
        grad_acc, route_acc = carry
        rows_idx, used, wg, wu, wd = pieces
        token_idx = (rows_idx // TOP).astype(jnp.int32)
        mask = used.astype(jnp.float32)
        xs = inputs[token_idx] * used.astype(jnp.bfloat16)[:, None]
        dys = out_grad[token_idx] * used.astype(jnp.bfloat16)[:, None]
        weights = flat_weight[rows_idx] * mask
        gate = jnp.dot(xs, wg.T, preferred_element_type=jnp.float32)
        up = jnp.dot(xs, wu.T, preferred_element_type=jnp.float32)
        sig = jax.nn.sigmoid(gate)
        act = gate * sig
        hidden = (act * up).astype(jnp.bfloat16)
        back = jnp.dot(dys, wd.T, preferred_element_type=jnp.float32)
        route_part = jnp.sum(hidden.astype(jnp.float32) * back, axis=1)
        grad_hidden = weights[:, None] * back
        scaled = (weights[:, None] * dys.astype(jnp.float32)).astype(jnp.bfloat16)
        gdown = jnp.dot(hidden.T, scaled, preferred_element_type=jnp.float32)
        d_gate = (grad_hidden * up * sig * (1.0 + gate * (1.0 - sig))).astype(jnp.bfloat16)
        d_up = (grad_hidden * act).astype(jnp.bfloat16)
        ggate = jnp.dot(d_gate.T, xs, preferred_element_type=jnp.float32)
        gup = jnp.dot(d_up.T, xs, preferred_element_type=jnp.float32)
        row_grad = jnp.dot(d_gate, wg, preferred_element_type=jnp.float32) + jnp.dot(d_up, wu, preferred_element_type=jnp.float32)
        grad_acc = grad_acc.at[token_idx].add(row_grad * mask[:, None])
        route_acc = route_acc.at[rows_idx].add(route_part * mask)
        return (grad_acc, route_acc), (ggate, gup, gdown)

    start = (jnp.zeros((TOKENS, D), jnp.float32), jnp.zeros((TOKENS * TOP,), jnp.float32))
    (grad_acc, route_acc), (grad_gate, grad_up, grad_down) = lax.scan(one_expert, start, (table, filled, w_gate, w_up, w_down))
    return grad_acc.astype(jnp.bfloat16), route_acc.reshape(TOKENS, TOP), grad_gate, grad_up, grad_down
```

```python
import jax
import jax.numpy as jnp
from jax import lax
from jax.experimental import pallas as pl
from jax.experimental.pallas import tpu as pltpu
from jax.sharding import Mesh
from jax.sharding import PartitionSpec as P

HIDDEN = ("hidden_0", "hidden_1")
BF = jnp.bfloat16
F32 = jnp.float32
TOK = 192
CAP = 72
NB = 16
SH = 180
ROWS = NB * CAP
W2 = 384
CH = 192
NC = ROWS // CH
MESH_ID = pl.DeviceIdType.MESH
NT = (((1,), (1,)), ((), ()))
TN = (((0,), (0,)), ((), ()))


def remote(src, dst, send, recv, device):
    return pltpu.make_async_remote_copy(
        src_ref=src, dst_ref=dst, send_sem=send, recv_sem=recv,
        device_id=device, device_id_type=MESH_ID,
    )


def dispatch_kernel(xd_ref, rows_ref, buf, acc, ring_send, sib_send, recv):
    e = lax.axis_index("expert")
    hx, hy = lax.axis_index("hidden_0"), lax.axis_index("hidden_1")
    z, core = e // 2, e % 2
    right = ((z + 1) % 8) * 2 + core
    left = ((z + 7) % 8) * 2 + core
    sib = z * 2 + 1 - core

    barrier = pltpu.get_barrier_semaphore()
    for peer in (right, left, sib):
        pl.semaphore_signal(barrier, inc=1, device_id=(peer, hx, hy), device_id_type=MESH_ID)
    pl.semaphore_wait(barrier, 3)

    half = TOK // 2

    def copy(step, h, block, target, send):
        rows = pl.ds(half * h, half)
        src = xd_ref.at[rows] if step == 0 else buf.at[block, rows]
        return remote(src, buf.at[block, rows], send, recv.at[block, h], (target, hx, hy))

    def origin(d):
        return ((z + d + 8) % 8) * 2 + core

    started = []

    def go(c):
        c.start()
        started.append(c)

    for h in range(2):
        go(copy(0, h, e, right, ring_send.at[0, 0, h]))
        go(copy(0, h, e, left, ring_send.at[1, 0, h]))
    for h in range(2):
        go(copy(0, h, e, sib, sib_send.at[0, h]))
    buf[e] = xd_ref[...]
    for s in range(1, 5):
        for way in range(2):
            block = origin(-s if way == 0 else s)
            for h in range(2):
                if s == 4 and h != way:
                    continue
                copy(1, h, block, right, ring_send.at[0, 0, 0]).wait_recv()
                if s < 3 or (s == 3 and h == way):
                    go(copy(1, h, block, (right, left)[way], ring_send.at[way, s, h]))
                k = s if way == 0 else 8 - s
                go(copy(1, h, block, sib, sib_send.at[k, h]))
    for d in range(8):
        block = ((z + d) % 8) * 2 + 1 - core
        for h in range(2):
            copy(1, h, block, right, ring_send.at[0, 0, 0]).wait_recv()

    lane = lax.broadcasted_iota(jnp.int32, (TOK, 128), 1)
    lower = (
        lax.broadcasted_iota(jnp.int32, (TOK, TOK), 0)
        > lax.broadcasted_iota(jnp.int32, (TOK, TOK), 1)
    ).astype(BF)
    ones = jnp.ones((128, 128), BF)
    ef = e.astype(F32)

    def one_block(b, carry):
        blk = buf[b]
        meta = blk[:, 128:256].astype(F32)
        hit = ((meta == ef) & (lane >= 52) & (lane < 56)).astype(F32).astype(BF)
        named = jnp.dot(hit, ones, preferred_element_type=F32)
        slot = jnp.dot(lower, named.astype(BF), preferred_element_type=F32)
        pick = ((slot == lane.astype(F32)) & (named > 0.5)).astype(F32).astype(BF)
        rows = lax.dot_general(pick, blk, TN, preferred_element_type=F32)
        acc[pl.ds(pl.multiple_of(b * CAP, 8), CAP), :] = rows[:CAP]
        return carry

    lax.fori_loop(0, NB, one_block, 0, unroll=4)
    rows_ref[...] = acc[...].astype(BF)
    for c in started:
        c.wait_send()


def dispatch(xd):
    return pl.pallas_call(
        dispatch_kernel,
        out_shape=jax.ShapeDtypeStruct((ROWS, W2), BF),
        in_specs=[pl.BlockSpec(memory_space=pltpu.VMEM)],
        out_specs=pl.BlockSpec(memory_space=pltpu.VMEM),
        scratch_shapes=[
            pltpu.VMEM((NB, TOK, W2), BF),
            pltpu.VMEM((ROWS, W2), F32),
            pltpu.SemaphoreType.DMA((2, 4, 2)),
            pltpu.SemaphoreType.DMA((8, 2)),
            pltpu.SemaphoreType.DMA((NB, 2)),
        ],
        compiler_params=pltpu.CompilerParams(
            collective_id=0, has_side_effects=True, vmem_limit_bytes=24 * 2**20
        ),
        name="dispatch",
    )(xd)


def expert_kernel(
    rows_ref, wg_ref, wu_ref, wd_ref,
    gg_ref, gu_ref, gd_ref, out_ref, route_ref,
    xd, wraw, wf, wb, part, fwd, near, quart, gsum, term, dgu_t, hw_t, rp, rp_all,
    w_sem, ag_send, ag_recv, rs_send, rs_recv, rt_send, rt_recv,
):
    e = lax.axis_index("expert")
    hx, hy = lax.axis_index("hidden_0"), lax.axis_index("hidden_1")
    me = hx * 4 + hy

    def peer(j):
        return (e, j // 4, j % 4)

    barrier = pltpu.get_barrier_semaphore()
    for d in range(1, NB):
        pl.semaphore_signal(barrier, inc=1, device_id=peer((me + d) % NB), device_id_type=MESH_ID)
    raw = [wg_ref, wu_ref, wd_ref]
    load = [pltpu.make_async_copy(raw[k], wraw.at[k % 2], w_sem.at[k]) for k in range(3)]
    load[0].start()
    load[1].start()
    pl.semaphore_wait(barrier, NB - 1)

    def place(c):
        odd = c % 2
        a = jnp.where(odd == 0, hx, hy)
        b = jnp.where(odd == 0, hy, hx)
        return odd, a, b

    def shard(odd, a, b):
        return jnp.where(odd == 0, a * 4 + b, b * 4 + a)

    def rows_of(c):
        return pl.ds(pl.multiple_of(c * CH, CH), CH)

    def ag(c, slot, to, k, own=False):
        src = rows_ref.at[rows_of(c)] if own else xd.at[slot, rows_of(c)]
        return remote(
            src, xd.at[slot, rows_of(c)], ag_send.at[c, k], ag_recv.at[c, slot], peer(to)
        )

    def ag_wait(c, slot):
        ag(c, slot, me, 0).wait_recv()

    def stage_a(c):
        odd, a, b = place(c)
        ag(c, me, shard(odd, (a + 1) % 4, b), 0, True).start()
        ag(c, me, shard(odd, (a + 3) % 4, b), 1, True).start()
        ag(c, me, shard(odd, a, (b + 1) % 4), 3, True).start()
        ag(c, me, shard(odd, a, (b + 3) % 4), 4, True).start()

    def stage_b(c):
        odd, a, b = place(c)
        from_left = shard(odd, (a + 3) % 4, b)
        from_right = shard(odd, (a + 1) % 4, b)
        flip = (c // 2) % 2
        ag_wait(c, from_left)
        ag_wait(c, from_right)
        ag(
            c, jnp.where(flip == 0, from_left, from_right),
            jnp.where(flip == 0, from_right, from_left), 2,
        ).start()
        up, down = shard(odd, a, (b + 1) % 4), shard(odd, a, (b + 3) % 4)
        ag(c, from_left, up, 5).start()
        ag(c, from_left, down, 6).start()
        ag(c, from_right, up, 7).start()
        ag(c, from_right, down, 8).start()

    def stage_c(c):
        odd, a, b = place(c)
        far = shard(odd, (a + 2) % 4, b)
        up, down = shard(odd, a, (b + 1) % 4), shard(odd, a, (b + 3) % 4)
        ag_wait(c, far)
        ag(c, far, up, 9).start()
        ag(c, far, down, 10).start()
        for k, da in ((11, 0), (12, 1)):
            slot = shard(odd, (a + da) % 4, (b + 3) % 4)
            ag_wait(c, slot)
            ag(c, slot, up, k).start()
        slot = shard(odd, (a + 3) % 4, (b + 1) % 4)
        ag_wait(c, slot)
        ag(c, slot, down, 13).start()

    def stage_d(c):
        odd, a, b = place(c)
        slot = shard(odd, (a + 2) % 4, (b + 1) % 4)
        ag_wait(c, slot)
        ag(c, slot, shard(odd, a, (b + 3) % 4), 14).start()

    def rs(c, src, dst, k, to):
        return remote(src, dst, rs_send.at[c, k], rs_recv.at[c, k], peer(to))

    def rs_copy(c, k):
        odd, a, b = place(c)
        right, left = shard(odd, (a + 1) % 4, b), shard(odd, (a + 3) % 4, b)
        up, down = shard(odd, a, (b + 1) % 4), shard(odd, a, (b + 3) % 4)
        ar, al, ao = (a + 1) % 4, (a + 3) % 4, (a + 2) % 4
        bu, bd, bo = (b + 1) % 4, (b + 3) % 4, (b + 2) % 4
        if k == 0:
            return rs(c, part.at[c, ao, 0], fwd.at[c, 0], k, right)
        if k == 1:
            return rs(c, part.at[c, ao, 1], fwd.at[c, 1], k, left)
        if k == 2:
            return rs(c, part.at[c, ar, 1], near.at[c, 0, 1], k, right)
        if k == 3:
            return rs(c, part.at[c, al, 0], near.at[c, 1, 0], k, left)
        if k == 4:
            return rs(c, part.at[c, ar, 0], near.at[c, 0, 0], k, right)
        if k == 5:
            return rs(c, part.at[c, al, 1], near.at[c, 1, 1], k, left)
        flip = (c // 2) % 2
        ahead, behind = jnp.where(flip == 0, up, down), jnp.where(flip == 0, down, up)
        ba, bb = jnp.where(flip == 0, bu, bd), jnp.where(flip == 0, bd, bu)
        if k == 6:
            return rs(c, quart.at[c, bo], gsum.at[c], k, ahead)
        if k == 7:
            return rs(c, quart.at[c, bb], term.at[c, 0], k, behind)
        return rs(c, quart.at[c, ba], term.at[c, 1], k, ahead)

    def stage_e(c):
        odd, a, b = place(c)
        rows = rows_of(c)
        bo = (b + 2) % 4
        for da in range(4):
            ag_wait(c, shard(odd, (a + da) % 4, bo))
        ag_wait(c, shard(odd, (a + 2) % 4, (b + 3) % 4))
        ag_wait(c, shard(odd, (a + 3) % 4, (b + 3) % 4))
        ag_wait(c, shard(odd, a, (b + 1) % 4))
        ag_wait(c, shard(odd, (a + 1) % 4, (b + 1) % 4))

        gate = up = back = None
        for s in range(NB):
            x = xd[s, rows, 0:256]
            y = xd[s, rows, 128:384]
            g1 = lax.dot_general(x, wf[0, s], NT, preferred_element_type=F32)
            u1 = lax.dot_general(x, wf[1, s], NT, preferred_element_type=F32)
            b1 = lax.dot_general(y, wf[2, s], NT, preferred_element_type=F32)
            gate = g1 if gate is None else gate + g1
            up = u1 if up is None else up + u1
            back = b1 if back is None else back + b1
        meta = xd[0, rows, 128:256].astype(F32)
        lane = lax.broadcasted_iota(jnp.int32, (CH, 128), 1)
        whole = pltpu.roll(meta, 124, 1) + pltpu.roll(meta, 120, 1)
        mine = (meta == e.astype(F32)) & (lane >= 52) & (lane < 56)
        w = jnp.sum(jnp.where(mine, whole, 0.0), axis=1, keepdims=True)
        sig = jax.nn.sigmoid(gate)
        act = gate * sig
        prod = act * up
        gh = w * back
        d_gate = gh * up * sig * (1.0 + gate * (1.0 - sig))
        d_up = gh * act
        hb = prod.astype(BF).astype(F32) * back
        hi = hb.astype(BF)
        lo = (hb - hi.astype(F32)).astype(BF)
        row8 = (lax.broadcasted_iota(jnp.int32, (8, CH), 0) == c).astype(F32).astype(BF)
        rp[:, 0:CH] += lax.dot_general(
            row8, hi, NT, preferred_element_type=F32
        ) + lax.dot_general(row8, lo, NT, preferred_element_type=F32)
        dgb, dub = d_gate.astype(BF), d_up.astype(BF)
        dgu_t[c, 0:192, :] = d_gate.T.astype(BF)
        dgu_t[c, 192:384, :] = d_up.T.astype(BF)
        hw_t[c] = (w * prod).T.astype(BF)
        for q in range(4):
            for h in range(2):
                lanes = slice(768 * q + 384 * h, 768 * q + 384 * h + 384)
                p = jnp.dot(dgb, wb[odd, 0, :, lanes], preferred_element_type=F32) + jnp.dot(
                    dub, wb[odd, 1, :, lanes], preferred_element_type=F32
                )
                part[c, q, h] = p.astype(BF)
        for k in range(4):
            rs_copy(c, k).start()

    def stage_f(c):
        odd, a, b = place(c)
        ar, al = (a + 1) % 4, (a + 3) % 4
        rs_copy(c, 0).wait_recv()
        part[c, ar, 0] = (part[c, ar, 0].astype(F32) + fwd[c, 0].astype(F32)).astype(BF)
        rs_copy(c, 4).start()
        rs_copy(c, 1).wait_recv()
        part[c, al, 1] = (part[c, al, 1].astype(F32) + fwd[c, 1].astype(F32)).astype(BF)
        rs_copy(c, 5).start()

    def stage_g(c):
        odd, a, b = place(c)
        for k in (2, 3, 4, 5):
            rs_copy(c, k).wait_recv()
        for h in range(2):
            q = (
                part[c, a, h].astype(F32) + near[c, 0, h].astype(F32) + near[c, 1, h].astype(F32)
            ).astype(BF)
            quart[c, 2 * h] = q[:, 0:256]
            quart[c, 2 * h + 1] = q[:, 128:384]
        rs_copy(c, 6).start()
        rs_copy(c, 7).start()

    def stage_h(c):
        odd, a, b = place(c)
        flip = (c // 2) % 2
        ba = jnp.where(flip == 0, (b + 1) % 4, (b + 3) % 4)
        rs_copy(c, 6).wait_recv()
        quart[c, ba] = (quart[c, ba].astype(F32) + gsum[c].astype(F32)).astype(BF)
        rs_copy(c, 8).start()

    def stage_i(c):
        odd, a, b = place(c)
        rs_copy(c, 7).wait_recv()
        rs_copy(c, 8).wait_recv()
        r = quart[c, b].astype(F32) + term[c, 0].astype(F32) + term[c, 1].astype(F32)
        r = jnp.where(b % 2 == 1, pltpu.roll(r, 192, 1), r)
        out_ref[rows_of(c), :] = r[:, 0:192].astype(BF)

    def guard(cond, f, *args):
        @pl.when(cond)
        def _():
            f(*args)

    stage_a(0)
    xd[me] = rows_ref[...]
    rp[...] = jnp.zeros_like(rp)
    wf[...] = jnp.zeros_like(wf)
    wb[...] = jnp.zeros_like(wb)
    for k in range(3):
        load[k].wait()
        for s in range(NB):
            w = wraw[k % 2, :, SH * s : SH * s + SH]
            at = 0 if k < 2 else 64
            wf[k, s, 0:SH, at : at + SH] = w
            if k < 2:
                t = (s % 4) * 4 + s // 4
                wb[0, k, 0:SH, 192 * s : 192 * s + SH] = w
                wb[1, k, 0:SH, 192 * t : 192 * t + SH] = w
        if k == 0:
            load[2].start()

    def step(t, carry):
        guard((t >= 1) & (t < NC), stage_a, t)
        guard((t >= 1) & (t < NC + 1), stage_b, t - 1)
        guard((t >= 2) & (t < NC + 2), stage_c, t - 2)
        guard((t >= 3) & (t < NC + 3), stage_d, t - 3)
        guard((t >= 5) & (t < NC + 5), stage_f, t - 5)
        guard((t >= 6) & (t < NC + 6), stage_g, t - 6)
        guard((t >= 7) & (t < NC + 7), stage_h, t - 7)
        guard((t >= 8) & (t < NC + 8), stage_i, t - 8)
        guard((t >= 4) & (t < NC + 4), stage_e, t - 4)
        return carry

    lax.fori_loop(0, NC + 4, step, 0)

    def rt(d):
        j = (me + d) % NB
        return remote(rp, rp_all.at[me], rt_send.at[d], rt_recv.at[me], peer(j))

    for d in range(1, NB):
        rt(d).start()
    rp_all[me] = rp[...]

    def weight_grads(s):
        gu = hd = None
        for c in range(NC):
            x = xd[s, CH * c : CH * c + CH, 0:256]
            y = xd[s, CH * c : CH * c + CH, 128:384]
            g1 = jnp.dot(dgu_t[c], x, preferred_element_type=F32)
            h1 = jnp.dot(hw_t[c], y, preferred_element_type=F32)
            gu = g1 if gu is None else gu + g1
            hd = h1 if hd is None else hd + h1
        lanes = slice(SH * s, SH * s + SH)
        gg_ref[:, lanes] = gu[0:SH, 0:SH]
        gu_ref[:, lanes] = gu[192 : 192 + SH, 0:SH]
        gd_ref[:, lanes] = hd[0:SH, 64 : 64 + SH]

    done = 0
    for t in range(NC + 4, NC + 8):
        for off, f in ((5, stage_f), (6, stage_g), (7, stage_h), (8, stage_i)):
            if t - off < NC:
                f(t - off)
        for s in range(done, done + 4):
            weight_grads(s)
        done += 4

    for d in range(1, NB):
        j = (me + d) % NB
        remote(rp, rp_all.at[j], rt_send.at[d], rt_recv.at[j], peer(j)).wait_recv()
    total = rp_all[0]
    for j in range(1, NB):
        total = total + rp_all[j]
    route_ref[...] = total

    for d in range(1, NB):
        rt(d).wait_send()

    def drain(c, carry):
        for k in range(15):
            ag(c, me, me, k, True).wait_send()
        for k in range(9):
            rs_copy(c, k).wait_send()
        return carry

    lax.fori_loop(0, NC, drain, 0)


def experts(rows, w_gate, w_up, w_down):
    vm = pl.BlockSpec(memory_space=pltpu.VMEM)
    hbm = pl.BlockSpec(memory_space=pl.ANY)
    grad = jax.ShapeDtypeStruct((SH, NB * SH), F32)
    return pl.pallas_call(
        expert_kernel,
        out_shape=[
            grad, grad, grad,
            jax.ShapeDtypeStruct((ROWS, 192), BF),
            jax.ShapeDtypeStruct((8, 256), F32),
        ],
        in_specs=[vm, hbm, hbm, hbm],
        out_specs=[vm] * 5,
        scratch_shapes=[
            pltpu.VMEM((NB, ROWS, W2), BF),
            pltpu.VMEM((2, SH, NB * SH), BF),
            pltpu.VMEM((3, NB, 192, 256), BF),
            pltpu.VMEM((2, 2, 192, NB * 192), BF),
            pltpu.VMEM((NC, 4, 2, CH, 384), BF),
            pltpu.VMEM((NC, 2, CH, 384), BF),
            pltpu.VMEM((NC, 2, 2, CH, 384), BF),
            pltpu.VMEM((NC, 4, CH, 256), BF),
            pltpu.VMEM((NC, CH, 256), BF),
            pltpu.VMEM((NC, 2, CH, 256), BF),
            pltpu.VMEM((NC, 384, CH), BF),
            pltpu.VMEM((NC, 192, CH), BF),
            pltpu.VMEM((8, 256), F32),
            pltpu.VMEM((NB, 8, 256), F32),
            pltpu.SemaphoreType.DMA((3,)),
            pltpu.SemaphoreType.DMA((NC, 15)),
            pltpu.SemaphoreType.DMA((NC, NB)),
            pltpu.SemaphoreType.DMA((NC, 9)),
            pltpu.SemaphoreType.DMA((NC, 9)),
            pltpu.SemaphoreType.DMA((NB,)),
            pltpu.SemaphoreType.DMA((NB,)),
        ],
        compiler_params=pltpu.CompilerParams(
            collective_id=1, has_side_effects=True, vmem_limit_bytes=67043328
        ),
        name="experts",
    )(rows, w_gate, w_up, w_down)


def per_device(inputs, out_grad, expert_ids, route_weight, w_gate, w_up, w_down):
    ids = expert_ids.astype(BF)
    w_hi = route_weight.astype(BF)
    w_lo = (route_weight - w_hi.astype(F32)).astype(BF)
    xd = jnp.concatenate(
        [inputs, ids, w_hi, w_lo, out_grad, jnp.zeros((TOK, W2 - 372), BF)], axis=1
    )
    rows = dispatch(xd)
    gg, gu, gd, back, route = experts(rows, w_gate[0], w_up[0], w_down[0])

    route = route[:NC, :CH].reshape(ROWS, 1)
    r_hi = route.astype(BF)
    r_lo = (route - r_hi.astype(F32)).astype(BF)
    send = jnp.concatenate([back[:, :SH], r_hi, r_lo], axis=1).reshape(NB, CAP, SH + 2)
    got = lax.all_to_all(send, "expert", split_axis=0, concat_axis=0, tiled=True)

    experts_ = jnp.arange(NB, dtype=jnp.int32)
    hit = expert_ids[:, :, None] == experts_[None, None, :]
    named = jnp.any(hit, axis=1).astype(F32)
    before = jnp.tril(jnp.ones((TOK, TOK), F32), -1)
    slot = jnp.dot(before, named, preferred_element_type=F32)
    at = slot[:, None, :, None] == jnp.arange(CAP, dtype=F32)[None, None, None, :]
    pick = (hit[:, :, :, None] & at).astype(BF).reshape(TOK, 4, ROWS)
    got = got.reshape(ROWS, SH + 2)
    mixed = jnp.einsum("tkr,rd->ktd", pick, got, preferred_element_type=F32)
    grad_input = jnp.sum(mixed[:, :, :SH], axis=0).astype(BF)
    grad_route = (mixed[:, :, SH] + mixed[:, :, SH + 1]).T
    return grad_input, grad_route, gg[None], gu[None], gd[None]


def solution(mesh):
    torus = Mesh(
        mesh.devices.reshape(mesh.shape["expert"], 4, 4), ("expert", "hidden_0", "hidden_1")
    )
    placed = (
        P("expert", HIDDEN),
        P("expert", HIDDEN),
        P("expert", None),
        P("expert", None),
        P("expert", HIDDEN, None),
        P("expert", HIDDEN, None),
        P("expert", HIDDEN, None),
    )
    return jax.shard_map(
        per_device,
        mesh=torus,
        in_specs=placed,
        out_specs=(
            P("expert", HIDDEN),
            P("expert", None),
            P("expert", HIDDEN, None),
            P("expert", HIDDEN, None),
            P("expert", HIDDEN, None),
        ),
        check_vma=False,
    )
```

```python
import jax
import jax.numpy as jnp
from jax import lax
from jax.experimental import pallas as pl
from jax.experimental.pallas import tpu as pltpu
from jax.sharding import Mesh
from jax.sharding import PartitionSpec as P

HIDDEN = ("hidden_0", "hidden_1")
BF = jnp.bfloat16
F32 = jnp.float32
TOK = 192
CAP = 72
NB = 16
SH = 180
ROWS = NB * CAP
W2 = 384
CH = 2 * CAP
NC = ROWS // CH
RET = 80
MESH_ID = pl.DeviceIdType.MESH
NT = (((1,), (1,)), ((), ()))
TN = (((0,), (0,)), ((), ()))


def remote(src, dst, send, recv, device):
    return pltpu.make_async_remote_copy(
        src_ref=src, dst_ref=dst, send_sem=send, recv_sem=recv,
        device_id=device, device_id_type=MESH_ID,
    )


def layer_kernel(
    x_ref, dy_ref, ids_ref, rw_ref, wg_ref, wu_ref, wd_ref,
    gg_ref, gu_ref, gd_ref, gin_ref, gr_ref,
    xin, buf, xd, wraw, wf, wb, part, fwd, near, quart, gsum, term, dgu_t, hw_t, rp, rp_all,
    ret, got, rsend, rgot, gacc, racc, grads, chosen,
    w_sem, z_send, z_recv, sib_recv, ag_send, ag_recv, rs_send, rs_recv, rt_send, rt_recv,
    ret_send, ret_recv, rr_send, rr_recv, g_sem,
):
    e = lax.axis_index("expert")
    hx, hy = lax.axis_index("hidden_0"), lax.axis_index("hidden_1")
    me = hx * 4 + hy
    z, core = e // 2, e % 2
    ef = e.astype(F32)

    def peer(j):
        return (e, j // 4, j % 4)

    def owner(j):
        return (j, hx, hy)

    barrier = pltpu.get_barrier_semaphore()
    for d in range(1, NB):
        pl.semaphore_signal(barrier, inc=1, device_id=peer((me + d) % NB), device_id_type=MESH_ID)
        pl.semaphore_signal(barrier, inc=1, device_id=owner((e + d) % NB), device_id_type=MESH_ID)
    raw = [wg_ref, wu_ref, wd_ref]
    load = [pltpu.make_async_copy(raw[k], wraw.at[k % 2], w_sem.at[k]) for k in range(3)]
    load[0].start()
    load[1].start()
    rw = rw_ref[...]
    w_hi = rw.astype(BF).astype(F32)
    xt = [x_ref[...].astype(F32), ids_ref[...].astype(F32), w_hi, rw - w_hi]
    xin[:, 0:192] = jnp.concatenate(xt, axis=0).T.astype(BF)
    yt = [dy_ref[...].astype(F32), jnp.zeros((192 - SH, TOK), F32)]
    xin[:, 192:384] = jnp.concatenate(yt, axis=0).T.astype(BF)
    pl.semaphore_wait(barrier, 2 * (NB - 1))

    right = ((z + 1) % 8) * 2 + core
    left = ((z + 7) % 8) * 2 + core
    sib = z * 2 + 1 - core
    half = TOK // 2

    def zcopy(first, h, block, target, recv):
        rows = pl.ds(half * h, half)
        src = xin.at[rows] if first else buf.at[block, rows]
        return remote(src, buf.at[block, rows], z_send.at[0], recv, owner(target))

    def zfirst():
        for h in range(2):
            zcopy(True, h, e, sib, sib_recv.at[0]).start()
        for h in range(2):
            zcopy(True, h, e, right, z_recv.at[0, 0]).start()
            zcopy(True, h, e, left, z_recv.at[0, 1]).start()

    def zwait(block, recv, n):
        at = buf.at[block, pl.ds(0, half * n)]
        remote(at, at, z_send.at[0], recv, owner(sib)).wait_recv()

    def zstage(s):
        for way in range(2):
            d = -s if way == 0 else s
            block = ((z + d + 8) % 8) * 2 + core
            zwait(block, z_recv.at[s - 1, way], 2 if s < 4 else 1)
            for h in range(2):
                if s == 4 and h != way:
                    continue
                if s < 3 or (s == 3 and h == way):
                    zcopy(False, h, block, (right, left)[way], z_recv.at[s, way]).start()
                zcopy(False, h, block, sib, sib_recv.at[s if way == 0 else 8 - s]).start()

    lane = lax.broadcasted_iota(jnp.int32, (TOK, 128), 1)
    id_lane = (lane >= 52) & (lane < 56)

    def picks(meta, expert):
        lower = (
            lax.broadcasted_iota(jnp.int32, (TOK, TOK), 0)
            > lax.broadcasted_iota(jnp.int32, (TOK, TOK), 1)
        ).astype(F32).astype(BF)
        hit = ((meta == expert) & id_lane).astype(F32).astype(BF)
        named = jnp.dot(hit, jnp.ones((128, 128), BF), preferred_element_type=F32)
        slot = jnp.dot(lower, named.astype(BF), preferred_element_type=F32)
        return ((slot == lane.astype(F32)) & (named > 0.5)).astype(F32).astype(BF)

    def rows_of(c):
        return pl.ds(pl.multiple_of(c * CH, 16), CH)

    def stage_x(c):
        plane = (z + c) % 8
        other = plane * 2 + 1 - core
        zwait(other, sib_recv.at[(8 - c) % 8], 2)
        pair = []
        for k in range(2):
            blk = buf[plane * 2 + k]
            pick = picks(blk[:, 128:256].astype(F32), ef)
            pair.append(lax.dot_general(pick, blk, TN, preferred_element_type=F32)[:CAP])
        xd[me, rows_of(c), :] = jnp.concatenate(pair, axis=0).astype(BF)

    def place(c):
        odd = c % 2
        a = jnp.where(odd == 0, hx, hy)
        b = jnp.where(odd == 0, hy, hx)
        return odd, a, b

    def shard(odd, a, b):
        return jnp.where(odd == 0, a * 4 + b, b * 4 + a)

    def ag(c, slot, to, k):
        at = xd.at[slot, rows_of(c)]
        group = 0 if k < 2 else 1 if k in (2, 3, 6, 7) else 2 if k == 10 else 3
        return remote(at, at, ag_send.at[c], ag_recv.at[c, group], peer(to))

    def ag_all(c, group, n):
        at = xd.at[pl.ds(0, n), rows_of(c)]
        return remote(at, at, ag_send.at[c], ag_recv.at[c, group], peer(me))

    def stage_a(c):
        odd, a, b = place(c)
        ag(c, me, shard(odd, (a + 1) % 4, b), 0).start()
        ag(c, me, shard(odd, (a + 3) % 4, b), 1).start()
        ag(c, me, shard(odd, a, (b + 1) % 4), 3).start()
        ag(c, me, shard(odd, a, (b + 3) % 4), 4).start()

    def stage_b(c):
        odd, a, b = place(c)
        from_left = shard(odd, (a + 3) % 4, b)
        from_right = shard(odd, (a + 1) % 4, b)
        flip = (c // 2) % 2
        ag_all(c, 0, 2).wait_recv()
        ag(
            c, jnp.where(flip == 0, from_left, from_right),
            jnp.where(flip == 0, from_right, from_left), 2,
        ).start()
        up, down = shard(odd, a, (b + 1) % 4), shard(odd, a, (b + 3) % 4)
        ag(c, from_left, up, 5).start()
        ag(c, from_left, down, 6).start()
        ag(c, from_right, up, 7).start()
        ag(c, from_right, down, 8).start()

    def stage_c(c):
        odd, a, b = place(c)
        far = shard(odd, (a + 2) % 4, b)
        up, down = shard(odd, a, (b + 1) % 4), shard(odd, a, (b + 3) % 4)
        ag_all(c, 1, 4).wait_recv()
        ag(c, far, up, 9).start()
        ag(c, far, down, 10).start()
        for k, da in ((11, 0), (12, 1)):
            slot = shard(odd, (a + da) % 4, (b + 3) % 4)
            ag(c, slot, up, k).start()
        slot = shard(odd, (a + 3) % 4, (b + 1) % 4)
        ag(c, slot, down, 13).start()

    def stage_d(c):
        odd, a, b = place(c)
        slot = shard(odd, (a + 2) % 4, (b + 1) % 4)
        ag_all(c, 2, 1).wait_recv()
        ag(c, slot, shard(odd, a, (b + 3) % 4), 14).start()

    def rs(c, src, dst, k, to):
        group = (0, 1, 2, 2, 2, 2, 3, 4, 4)[k]
        return remote(src, dst, rs_send.at[c, k // 6], rs_recv.at[c, group], peer(to))

    def rs_copy(c, k):
        odd, a, b = place(c)
        right, left = shard(odd, (a + 1) % 4, b), shard(odd, (a + 3) % 4, b)
        up, down = shard(odd, a, (b + 1) % 4), shard(odd, a, (b + 3) % 4)
        ar, al, ao = (a + 1) % 4, (a + 3) % 4, (a + 2) % 4
        bu, bd, bo = (b + 1) % 4, (b + 3) % 4, (b + 2) % 4
        if k == 0:
            return rs(c, part.at[c, ao, 0], fwd.at[c, 0], k, right)
        if k == 1:
            return rs(c, part.at[c, ao, 1], fwd.at[c, 1], k, left)
        if k == 2:
            return rs(c, part.at[c, ar, 1], near.at[c, 0, 1], k, right)
        if k == 3:
            return rs(c, part.at[c, al, 0], near.at[c, 1, 0], k, left)
        if k == 4:
            return rs(c, part.at[c, ar, 0], near.at[c, 0, 0], k, right)
        if k == 5:
            return rs(c, part.at[c, al, 1], near.at[c, 1, 1], k, left)
        flip = (c // 2) % 2
        ahead, behind = jnp.where(flip == 0, up, down), jnp.where(flip == 0, down, up)
        ba, bb = jnp.where(flip == 0, bu, bd), jnp.where(flip == 0, bd, bu)
        if k == 6:
            return rs(c, quart.at[c, bo], gsum.at[c], k, ahead)
        if k == 7:
            return rs(c, quart.at[c, bb], term.at[c, 0], k, behind)
        return rs(c, quart.at[c, ba], term.at[c, 1], k, ahead)

    def stage_e(c):
        odd, a, b = place(c)
        rows = rows_of(c)
        ag_all(c, 3, 8).wait_recv()

        gate = up = back = None
        for s in range(NB):
            x = xd[s, rows, 0:256]
            y = xd[s, rows, 128:384]
            g1 = lax.dot_general(x, wf[0, s], NT, preferred_element_type=F32)
            u1 = lax.dot_general(x, wf[1, s], NT, preferred_element_type=F32)
            b1 = lax.dot_general(y, wf[2, s], NT, preferred_element_type=F32)
            gate = g1 if gate is None else gate + g1
            up = u1 if up is None else up + u1
            back = b1 if back is None else back + b1
        meta = xd[0, rows, 128:256].astype(F32)
        lane = lax.broadcasted_iota(jnp.int32, (CH, 128), 1)
        whole = pltpu.roll(meta, 124, 1) + pltpu.roll(meta, 120, 1)
        mine = (meta == e.astype(F32)) & (lane >= 52) & (lane < 56)
        w = jnp.sum(jnp.where(mine, whole, 0.0), axis=1, keepdims=True)
        sig = jax.nn.sigmoid(gate)
        act = gate * sig
        prod = act * up
        gh = w * back
        d_gate = gh * up * sig * (1.0 + gate * (1.0 - sig))
        d_up = gh * act
        hb = prod.astype(BF).astype(F32) * back
        hi = hb.astype(BF)
        lo = (hb - hi.astype(F32)).astype(BF)
        row8 = (lax.broadcasted_iota(jnp.int32, (8, 192), 0) == c).astype(F32).astype(BF)
        rp[:, 0:CH] += lax.dot_general(
            row8, hi, NT, preferred_element_type=F32
        ) + lax.dot_general(row8, lo, NT, preferred_element_type=F32)
        dgb, dub = d_gate.astype(BF), d_up.astype(BF)
        dgu_t[c, 0:192, :] = d_gate.T.astype(BF)
        dgu_t[c, 192:384, :] = d_up.T.astype(BF)
        hw_t[c] = (w * prod).T.astype(BF)
        for q in range(4):
            for h in range(2):
                lanes = slice(768 * q + 384 * h, 768 * q + 384 * h + 384)
                p = jnp.dot(dgb, wb[odd, 0, :, lanes], preferred_element_type=F32) + jnp.dot(
                    dub, wb[odd, 1, :, lanes], preferred_element_type=F32
                )
                part[c, q, h] = p.astype(BF)
        for k in range(4):
            rs_copy(c, k).start()

    def stage_f(c):
        odd, a, b = place(c)
        ar, al = (a + 1) % 4, (a + 3) % 4
        rs_copy(c, 0).wait_recv()
        part[c, ar, 0] = (part[c, ar, 0].astype(F32) + fwd[c, 0].astype(F32)).astype(BF)
        rs_copy(c, 4).start()
        rs_copy(c, 1).wait_recv()
        part[c, al, 1] = (part[c, al, 1].astype(F32) + fwd[c, 1].astype(F32)).astype(BF)
        rs_copy(c, 5).start()

    def stage_g(c):
        odd, a, b = place(c)
        at = near.at[c]
        remote(at, at, rs_send.at[c, 0], rs_recv.at[c, 2], peer(me)).wait_recv()
        for h in range(2):
            q = (
                part[c, a, h].astype(F32) + near[c, 0, h].astype(F32) + near[c, 1, h].astype(F32)
            ).astype(BF)
            quart[c, 2 * h] = q[:, 0:256]
            quart[c, 2 * h + 1] = q[:, 128:384]
        rs_copy(c, 6).start()
        rs_copy(c, 7).start()

    def stage_h(c):
        odd, a, b = place(c)
        flip = (c // 2) % 2
        ba = jnp.where(flip == 0, (b + 1) % 4, (b + 3) % 4)
        rs_copy(c, 6).wait_recv()
        quart[c, ba] = (quart[c, ba].astype(F32) + gsum[c].astype(F32)).astype(BF)
        rs_copy(c, 8).start()

    def back_copy(c, k, src, dst, send, recv, split):
        at = src.at[c, k] if split else src.at[c]
        to = ((z + c) % 8) * 2 + k
        return remote(at, dst.at[e], send.at[0], recv.at[c if split else 0], owner(to))

    def send_back(c, src, dst, send, recv, split):
        @pl.when(c > 0)
        def _():
            back_copy(c, 0, src, dst, send, recv, split).start()
            back_copy(c, 1, src, dst, send, recv, split).start()

        @pl.when(c == 0)
        def _():
            back_copy(c, 1 - core, src, dst, send, recv, split).start()
            dst[e] = src[c, core] if split else src[c]

    def back_all(n, dst, send, recv):
        at = dst.at[pl.ds(0, n)]
        return remote(at, at, send.at[0], recv, owner(sib))

    def stage_i(c):
        odd, a, b = place(c)
        at = term.at[c]
        remote(at, at, rs_send.at[c, 1], rs_recv.at[c, 4], peer(me)).wait_recv()
        r = quart[c, b].astype(F32) + term[c, 0].astype(F32) + term[c, 1].astype(F32)
        r = jnp.where(b % 2 == 1, pltpu.roll(r, 192, 1), r)
        pad = jnp.zeros((RET - CAP, 256), F32)
        ret[c, 0] = jnp.concatenate([r[0:CAP], pad], axis=0).astype(BF)
        ret[c, 1] = jnp.concatenate([r[CAP:CH], pad], axis=0).astype(BF)
        send_back(c, ret, got, ret_send, ret_recv, True)

    def choose(first, last):
        def one(j, carry):
            chosen[j] = picks(xin[:, 128:256].astype(F32), j.astype(F32))
            return carry

        lax.fori_loop(first, last, one, 0, unroll=4)

    def stage_j(c):
        @pl.when(c > 0)
        def _():
            back_all(2, got, ret_send, ret_recv.at[c]).wait_recv()

        @pl.when(c == 0)
        def _():
            back_all(1, got, ret_send, ret_recv.at[c]).wait_recv()

        total = gacc[...]
        for k in range(2):
            j = ((z + 8 - c) % 8) * 2 + k
            total = total + jnp.dot(
                chosen[j, :, 0:RET], got[j], preferred_element_type=F32
            )
        gacc[...] = total

    def routes(c):
        meta = xin[:, 128:256].astype(F32)
        total = racc[...]
        for k in range(2):
            j = ((z + 8 - c) % 8) * 2 + k
            r = rgot[j]
            r = jnp.where(core == 1, pltpu.roll(r, 256 - CAP, 1), r)[:, 0:128]
            hi = r.astype(BF).astype(F32)
            row = lax.broadcasted_iota(jnp.int32, (8, 128), 0)
            both = jnp.where(row == 0, hi, jnp.where(row == 1, r - hi, 0.0)).astype(BF)
            value = jnp.sum(
                lax.dot_general(chosen[j], both, NT, preferred_element_type=F32),
                axis=1, keepdims=True,
            )
            total = total + jnp.where((meta == j.astype(F32)) & id_lane, value, 0.0)
        racc[...] = total

    def guard(cond, f, *args):
        @pl.when(cond)
        def _():
            with jax.named_scope(f.__name__):
                f(*args)

    def prepare(k):
        load[k].wait()
        for s in range(NB):
            w = wraw[k % 2, :, SH * s : SH * s + SH]
            at = 0 if k < 2 else 64
            wf[k, s, 0:SH, at : at + SH] = w
            if k < 2:
                t = (s % 4) * 4 + s // 4
                wb[0, k, 0:SH, 192 * s : 192 * s + SH] = w
                wb[1, k, 0:SH, 192 * t : 192 * t + SH] = w
        if k == 0:
            load[2].start()

    def drain_ag(c):
        ag_all(c, 0, 15).wait_send()

    def drain_ag(c):
        ag_all(c, 0, 15).wait_send()

    def drain_rs(c):
        at = part.at[c, pl.ds(0, 3)]
        remote(at, at, rs_send.at[c, 0], rs_recv.at[c, 0], peer(me)).wait_send()
        at = quart.at[c, pl.ds(0, 3)]
        remote(at, at, rs_send.at[c, 1], rs_recv.at[c, 0], peer(me)).wait_send()

    zfirst()
    buf[e] = xin[...]
    stage_x(0)
    stage_a(0)
    rp[...] = jnp.zeros_like(rp)
    gacc[...] = jnp.zeros_like(gacc)
    racc[...] = jnp.zeros_like(racc)
    wf[...] = jnp.zeros_like(wf)
    wb[...] = jnp.zeros_like(wb)
    prepare(0)
    stage_b(0)
    zstage(1)
    stage_x(1)
    stage_a(1)
    prepare(1)
    choose(0, 8)
    stage_c(0)
    stage_b(1)
    zstage(2)
    stage_x(2)
    stage_a(2)
    stage_d(0)
    prepare(2)
    choose(8, 16)
    zstage(3)
    stage_c(1)
    zstage(4)

    def step(t, carry):
        guard(t < NC - 1, stage_x, t + 1)
        guard(t < NC - 1, stage_a, t + 1)
        guard(t >= 2, stage_b, t)
        guard(t >= 2, stage_d, t - 1)
        guard(t >= 3, stage_f, t - 3)
        guard(t >= 2, stage_e, t - 2)
        guard(t >= 2, stage_c, t)
        guard(t >= 3, stage_g, t - 3)
        guard(t >= 4, stage_h, t - 4)
        guard(t >= 5, stage_i, t - 5)
        guard(t >= 6, stage_j, t - 6)
        guard(t >= 4, drain_ag, t - 4)
        guard(t >= 6, drain_rs, t - 6)
        return carry

    lax.fori_loop(2, NC, step, 0)

    def rt(d):
        j = (me + d) % NB
        return remote(rp, rp_all.at[me], rt_send.at[0], rt_recv.at[0], peer(j))

    def rt_all():
        at = rp_all.at[pl.ds(0, NB - 1)]
        return remote(at, at, rt_send.at[0], rt_recv.at[0], peer(me))

    def routes_out():
        for d in range(1, NB):
            rt(d).start()
        rp_all[me] = rp[...]

    def routes_back():
        rt_all().wait_recv()
        total = rp_all[0]
        for j in range(1, NB):
            total = total + rp_all[j]
        for k in range(NC):
            rsend[k] = jnp.broadcast_to(total[k : k + 1, :], (8, 256))
            send_back(k, rsend, rgot, rr_send, rr_recv, False)

    def weight_grads(s):
        gu = hd = None
        for c in range(NC):
            x = xd[s, CH * c : CH * c + CH, 0:256]
            y = xd[s, CH * c : CH * c + CH, 128:384]
            g1 = jnp.dot(dgu_t[c], x, preferred_element_type=F32)
            h1 = jnp.dot(hw_t[c], y, preferred_element_type=F32)
            gu = g1 if gu is None else gu + g1
            hd = h1 if hd is None else hd + h1
        lanes = slice(SH * s, SH * s + SH)
        grads[0, :, lanes] = gu[0:SH, 0:SH]
        grads[1, :, lanes] = gu[192 : 192 + SH, 0:SH]
        grads[2, :, lanes] = hd[0:SH, 64 : 64 + SH]

    def grad_copy(k, i):
        lanes = slice((0, 1152, 1920)[i], (1152, 1920, 2880)[i])
        out = (gg_ref, gu_ref, gd_ref)[k]
        return pltpu.make_async_copy(grads.at[k, :, lanes], out.at[:, 0, lanes], g_sem.at[k])

    def wg(first, last):
        with jax.named_scope("wg"):
            for s in range(first, last):
                weight_grads(s)

    def tail(f, c):
        with jax.named_scope(f.__name__):
            f(c)

    def grads_out(i):
        for k in range(3):
            grad_copy(k, i).start()

    tail(stage_d, 7)
    tail(stage_f, 5)
    tail(stage_e, 6)
    tail(stage_g, 5)
    tail(stage_h, 4)
    tail(stage_i, 3)
    tail(stage_j, 2)
    tail(stage_e, 7)
    routes_out()
    tail(stage_f, 6)
    drain_ag(4)
    wg(0, 4)
    tail(stage_h, 5)
    tail(stage_g, 6)
    tail(stage_f, 7)
    tail(stage_i, 4)
    tail(stage_j, 3)
    wg(4, 7)
    grads_out(0)
    tail(stage_h, 6)
    tail(stage_i, 5)
    tail(stage_j, 4)
    wg(7, 9)
    tail(stage_g, 7)
    routes_back()
    wg(9, 11)
    grads_out(1)
    tail(stage_i, 6)
    tail(stage_h, 7)
    tail(stage_j, 5)
    wg(11, 16)
    grads_out(2)
    tail(stage_i, 7)
    tail(stage_j, 6)
    back_all(NB - 1, rgot, rr_send, rr_recv.at[0]).wait_recv()
    for k in range(NC):
        tail(routes, k)
    gr_ref[...] = racc[...].T[52:56]
    with jax.named_scope("drain"):
        for k in range(5, NC):
            drain_ag(k)
        for k in range(2, NC):
            drain_rs(k)
        rt_all().wait_send()
        at = buf.at[pl.ds(0, 15)]
        remote(at, at, z_send.at[0], z_recv.at[0, 0], owner(sib)).wait_send()
        back_all(NB - 1, rgot, rr_send, rr_recv.at[0]).wait_send()
    with jax.named_scope("grads"):
        for k in range(3):
            out = (gg_ref, gu_ref, gd_ref)[k]
            pltpu.make_async_copy(grads.at[k], out.at[:, 0], g_sem.at[k]).wait()
    tail(stage_j, 7)
    back_all(NB - 1, got, ret_send, ret_recv.at[0]).wait_send()
    with jax.named_scope("gin"):
        gin_ref[...] = gacc[...].T[0:SH].astype(BF)


def layer(x, dy, ids, rw, w_gate, w_up, w_down):
    vm = pl.BlockSpec(memory_space=pltpu.VMEM)
    hbm = pl.BlockSpec(memory_space=pl.ANY)
    grad = jax.ShapeDtypeStruct((SH, 1, NB * SH), F32)
    dma = pltpu.SemaphoreType.DMA
    return pl.pallas_call(
        layer_kernel,
        out_shape=[
            grad, grad, grad,
            jax.ShapeDtypeStruct((SH, TOK), BF),
            jax.ShapeDtypeStruct((4, TOK), F32),
        ],
        in_specs=[vm] * 4 + [hbm] * 3,
        out_specs=[hbm] * 3 + [vm] * 2,
        scratch_shapes=[
            pltpu.VMEM((TOK, W2), BF),
            pltpu.VMEM((NB, TOK, W2), BF),
            pltpu.VMEM((NB, ROWS, W2), BF),
            pltpu.VMEM((2, SH, NB * SH), BF),
            pltpu.VMEM((3, NB, 192, 256), BF),
            pltpu.VMEM((2, 2, 192, NB * 192), BF),
            pltpu.VMEM((NC, 4, 2, CH, 384), BF),
            pltpu.VMEM((NC, 2, CH, 384), BF),
            pltpu.VMEM((NC, 2, 2, CH, 384), BF),
            pltpu.VMEM((NC, 4, CH, 256), BF),
            pltpu.VMEM((NC, CH, 256), BF),
            pltpu.VMEM((NC, 2, CH, 256), BF),
            pltpu.VMEM((NC, 384, CH), BF),
            pltpu.VMEM((NC, 192, CH), BF),
            pltpu.VMEM((8, 256), F32),
            pltpu.VMEM((NB, 8, 256), F32),
            pltpu.VMEM((NC, 2, RET, 256), BF),
            pltpu.VMEM((NB, RET, 256), BF),
            pltpu.VMEM((NC, 8, 256), F32),
            pltpu.VMEM((NB, 8, 256), F32),
            pltpu.VMEM((TOK, 256), F32),
            pltpu.VMEM((TOK, 128), F32),
            pltpu.VMEM((3, SH, NB * SH), F32),
            pltpu.VMEM((NB, TOK, 128), BF),
            dma((3,)),
            dma((1,)),
            dma((4, 2)),
            dma((8,)),
            dma((NC,)),
            dma((NC, 4)),
            dma((NC, 2)),
            dma((NC, 5)),
            dma((1,)),
            dma((1,)),
            dma((1,)),
            dma((NC,)),
            dma((1,)),
            dma((1,)),
            dma((3,)),
        ],
        compiler_params=pltpu.CompilerParams(
            collective_id=0, has_side_effects=True, vmem_limit_bytes=67043328
        ),
        name="layer",
    )(x, dy, ids, rw, w_gate, w_up, w_down)


def finish_kernel(g0, g1, g2, gin_ref, gr_ref, o0, o1, o2, ogin_ref, ogr_ref, held, sem):
    rows = SH // 6

    def piece(k, i, out):
        part = pl.ds(rows * i, rows)
        inner = held.at[k, part]
        outer = ((o0, o1, o2) if out else (g0, g1, g2))[k].at[part]
        src, dst = (inner, outer) if out else (outer, inner)
        return pltpu.make_async_copy(src, dst, sem.at[out, k, i])

    for k in range(3):
        for i in range(6):
            piece(k, i, 0).start()
    ogin_ref[...] = gin_ref[...]
    ogr_ref[...] = gr_ref[...]
    for k in range(3):
        for i in range(6):
            piece(k, i, 0).wait()
            piece(k, i, 1).start()
    for k in range(3):
        for i in range(6):
            piece(k, i, 1).wait()


def finish(*arrays):
    vm = pl.BlockSpec(memory_space=pltpu.VMEM)
    hbm = pl.BlockSpec(memory_space=pl.ANY)
    return pl.pallas_call(
        finish_kernel,
        out_shape=[jax.ShapeDtypeStruct(a.shape, a.dtype) for a in arrays],
        in_specs=[hbm] * 3 + [vm] * 2,
        out_specs=[hbm] * 3 + [vm] * 2,
        scratch_shapes=[
            pltpu.VMEM((3, SH, 1, NB * SH), F32),
            pltpu.SemaphoreType.DMA((2, 3, 6)),
        ],
        name="finish",
    )(*arrays)


def per_device(inputs, out_grad, expert_ids, route_weight, w_gate, w_up, w_down):
    found = layer(
        inputs.T, out_grad.T, expert_ids.T, route_weight.T, w_gate[0], w_up[0], w_down[0]
    )
    gg, gu, gd, grad_input, grad_route = finish(*found)
    grads = [jnp.transpose(g, (1, 0, 2)) for g in (gg, gu, gd)]
    return (grad_input.T, grad_route.T, *grads)


def solution(mesh):
    torus = Mesh(
        mesh.devices.reshape(mesh.shape["expert"], 4, 4), ("expert", "hidden_0", "hidden_1")
    )
    placed = (
        P("expert", HIDDEN),
        P("expert", HIDDEN),
        P("expert", None),
        P("expert", None),
        P("expert", HIDDEN, None),
        P("expert", HIDDEN, None),
        P("expert", HIDDEN, None),
    )
    return jax.shard_map(
        per_device,
        mesh=torus,
        in_specs=placed,
        out_specs=(
            P("expert", HIDDEN),
            P("expert", None),
            P("expert", HIDDEN, None),
            P("expert", HIDDEN, None),
            P("expert", HIDDEN, None),
        ),
        check_vma=False,
    )
```

```python
import jax
import jax.numpy as jnp
from jax import lax
from jax.experimental import pallas as pl
from jax.experimental.pallas import tpu as pltpu
from jax.sharding import Mesh
from jax.sharding import PartitionSpec as P

HIDDEN = ("hidden_0", "hidden_1")
BF = jnp.bfloat16
F32 = jnp.float32
TOK = 192
CAP = 72
NB = 16
SH = 180
ROWS = NB * CAP
W2 = 384
CH = 2 * CAP
NC = ROWS // CH
RET = 80
MESH_ID = pl.DeviceIdType.MESH
NT = (((1,), (1,)), ((), ()))
TN = (((0,), (0,)), ((), ()))


def remote(src, dst, send, recv, device):
    return pltpu.make_async_remote_copy(
        src_ref=src, dst_ref=dst, send_sem=send, recv_sem=recv,
        device_id=device, device_id_type=MESH_ID,
    )


def layer_kernel(
    x_ref, dy_ref, ids_ref, rw_ref, wg_ref, wu_ref, wd_ref,
    gg_ref, gu_ref, gd_ref, gin_ref, gr_ref,
    xin, buf, xd, wraw, wf, wb, part, fwd, near, quart, gsum, term, dgu_t, hw_t, rp, rp_all,
    ret, got, rsend, rgot, gacc, racc, grads, chosen,
    w_sem, z_send, z_recv, sib_recv, ag_send, ag_recv, rs_send, rs_recv, rt_send, rt_recv,
    ret_send, ret_recv, rr_send, rr_recv, g_sem,
):
    e = lax.axis_index("expert")
    hx, hy = lax.axis_index("hidden_0"), lax.axis_index("hidden_1")
    me = hx * 4 + hy
    z, core = e // 2, e % 2
    ef = e.astype(F32)

    def peer(j):
        return (e, j // 4, j % 4)

    def owner(j):
        return (j, hx, hy)

    barrier = pltpu.get_barrier_semaphore()
    for d in range(1, NB):
        pl.semaphore_signal(barrier, inc=1, device_id=peer((me + d) % NB), device_id_type=MESH_ID)
        pl.semaphore_signal(barrier, inc=1, device_id=owner((e + d) % NB), device_id_type=MESH_ID)
    raw = [wg_ref, wu_ref, wd_ref]
    load = [pltpu.make_async_copy(raw[k], wraw.at[k % 2], w_sem.at[k]) for k in range(3)]
    load[0].start()
    load[1].start()
    rw = rw_ref[...]
    w_hi = rw.astype(BF).astype(F32)
    xt = [x_ref[...].astype(F32), ids_ref[...].astype(F32), w_hi, rw - w_hi]
    xin[:, 0:192] = jnp.concatenate(xt, axis=0).T.astype(BF)
    yt = [dy_ref[...].astype(F32), jnp.zeros((192 - SH, TOK), F32)]
    xin[:, 192:384] = jnp.concatenate(yt, axis=0).T.astype(BF)
    pl.semaphore_wait(barrier, 2 * (NB - 1))

    right = ((z + 1) % 8) * 2 + core
    left = ((z + 7) % 8) * 2 + core
    sib = z * 2 + 1 - core
    half = TOK // 2

    def zcopy(first, h, block, target, recv):
        rows = pl.ds(half * h, half)
        src = xin.at[rows] if first else buf.at[block, rows]
        return remote(src, buf.at[block, rows], z_send.at[0], recv, owner(target))

    def zfirst():
        for h in range(2):
            zcopy(True, h, e, sib, sib_recv.at[0]).start()
        for h in range(2):
            zcopy(True, h, e, right, z_recv.at[0, 0]).start()
            zcopy(True, h, e, left, z_recv.at[0, 1]).start()

    def zwait(block, recv, n):
        at = buf.at[block, pl.ds(0, half * n)]
        remote(at, at, z_send.at[0], recv, owner(sib)).wait_recv()

    def zstage(s):
        for way in range(2):
            d = -s if way == 0 else s
            block = ((z + d + 8) % 8) * 2 + core
            zwait(block, z_recv.at[s - 1, way], 2 if s < 4 else 1)
            for h in range(2):
                if s == 4 and h != way:
                    continue
                if s < 3 or (s == 3 and h == way):
                    zcopy(False, h, block, (right, left)[way], z_recv.at[s, way]).start()
                zcopy(False, h, block, sib, sib_recv.at[s if way == 0 else 8 - s]).start()

    lane = lax.broadcasted_iota(jnp.int32, (TOK, 128), 1)
    id_lane = (lane >= 52) & (lane < 56)

    def picks(meta, expert):
        lower = (
            lax.broadcasted_iota(jnp.int32, (TOK, TOK), 0)
            > lax.broadcasted_iota(jnp.int32, (TOK, TOK), 1)
        ).astype(F32).astype(BF)
        hit = ((meta == expert) & id_lane).astype(F32).astype(BF)
        named = jnp.dot(hit, jnp.ones((128, 128), BF), preferred_element_type=F32)
        slot = jnp.dot(lower, named.astype(BF), preferred_element_type=F32)
        return ((slot == lane.astype(F32)) & (named > 0.5)).astype(F32).astype(BF)

    def rows_of(c):
        return pl.ds(pl.multiple_of(c * CH, 16), CH)

    def stage_x(c):
        plane = (z + c) % 8
        other = plane * 2 + 1 - core
        zwait(other, sib_recv.at[(8 - c) % 8], 2)
        pair = []
        for k in range(2):
            blk = buf[plane * 2 + k]
            pick = picks(blk[:, 128:256].astype(F32), ef)
            pair.append(lax.dot_general(pick, blk, TN, preferred_element_type=F32)[:CAP])
        xd[me, rows_of(c), :] = jnp.concatenate(pair, axis=0).astype(BF)

    def place(c):
        odd = c % 2
        a = jnp.where(odd == 0, hx, hy)
        b = jnp.where(odd == 0, hy, hx)
        return odd, a, b

    def shard(odd, a, b):
        return jnp.where(odd == 0, a * 4 + b, b * 4 + a)

    def ag(c, slot, to, k):
        at = xd.at[slot, rows_of(c)]
        group = 0 if k < 2 else 1 if k in (2, 3, 6, 7) else 2 if k == 10 else 3
        return remote(at, at, ag_send.at[c], ag_recv.at[c, group], peer(to))

    def ag_all(c, group, n):
        at = xd.at[pl.ds(0, n), rows_of(c)]
        return remote(at, at, ag_send.at[c], ag_recv.at[c, group], peer(me))

    def stage_a(c):
        odd, a, b = place(c)
        ag(c, me, shard(odd, (a + 1) % 4, b), 0).start()
        ag(c, me, shard(odd, (a + 3) % 4, b), 1).start()
        ag(c, me, shard(odd, a, (b + 1) % 4), 3).start()
        ag(c, me, shard(odd, a, (b + 3) % 4), 4).start()

    def stage_b(c):
        odd, a, b = place(c)
        from_left = shard(odd, (a + 3) % 4, b)
        from_right = shard(odd, (a + 1) % 4, b)
        flip = (c // 2) % 2
        ag_all(c, 0, 2).wait_recv()
        ag(
            c, jnp.where(flip == 0, from_left, from_right),
            jnp.where(flip == 0, from_right, from_left), 2,
        ).start()
        up, down = shard(odd, a, (b + 1) % 4), shard(odd, a, (b + 3) % 4)
        ag(c, from_left, up, 5).start()
        ag(c, from_left, down, 6).start()
        ag(c, from_right, up, 7).start()
        ag(c, from_right, down, 8).start()

    def stage_c(c):
        odd, a, b = place(c)
        far = shard(odd, (a + 2) % 4, b)
        up, down = shard(odd, a, (b + 1) % 4), shard(odd, a, (b + 3) % 4)
        ag_all(c, 1, 4).wait_recv()
        ag(c, far, up, 9).start()
        ag(c, far, down, 10).start()
        for k, da in ((11, 0), (12, 1)):
            slot = shard(odd, (a + da) % 4, (b + 3) % 4)
            ag(c, slot, up, k).start()
        slot = shard(odd, (a + 3) % 4, (b + 1) % 4)
        ag(c, slot, down, 13).start()

    def stage_d(c):
        odd, a, b = place(c)
        slot = shard(odd, (a + 2) % 4, (b + 1) % 4)
        ag_all(c, 2, 1).wait_recv()
        ag(c, slot, shard(odd, a, (b + 3) % 4), 14).start()

    def rs(c, src, dst, k, to):
        group = (0, 1, 2, 2, 2, 2, 3, 4, 4)[k]
        return remote(src, dst, rs_send.at[c, k // 6], rs_recv.at[c, group], peer(to))

    def rs_copy(c, k):
        odd, a, b = place(c)
        right, left = shard(odd, (a + 1) % 4, b), shard(odd, (a + 3) % 4, b)
        up, down = shard(odd, a, (b + 1) % 4), shard(odd, a, (b + 3) % 4)
        ar, al, ao = (a + 1) % 4, (a + 3) % 4, (a + 2) % 4
        bu, bd, bo = (b + 1) % 4, (b + 3) % 4, (b + 2) % 4
        if k == 0:
            return rs(c, part.at[c, ao, 0], fwd.at[c, 0], k, right)
        if k == 1:
            return rs(c, part.at[c, ao, 1], fwd.at[c, 1], k, left)
        if k == 2:
            return rs(c, part.at[c, ar, 1], near.at[c, 0, 1], k, right)
        if k == 3:
            return rs(c, part.at[c, al, 0], near.at[c, 1, 0], k, left)
        if k == 4:
            return rs(c, part.at[c, ar, 0], near.at[c, 0, 0], k, right)
        if k == 5:
            return rs(c, part.at[c, al, 1], near.at[c, 1, 1], k, left)
        flip = (c // 2) % 2
        ahead, behind = jnp.where(flip == 0, up, down), jnp.where(flip == 0, down, up)
        ba, bb = jnp.where(flip == 0, bu, bd), jnp.where(flip == 0, bd, bu)
        if k == 6:
            return rs(c, quart.at[c, bo], gsum.at[c], k, ahead)
        if k == 7:
            return rs(c, quart.at[c, bb], term.at[c, 0], k, behind)
        return rs(c, quart.at[c, ba], term.at[c, 1], k, ahead)

    def stage_e(c):
        odd, a, b = place(c)
        rows = rows_of(c)
        ag_all(c, 3, 8).wait_recv()

        gate = up = back = None
        for s in range(NB):
            x = xd[s, rows, 0:256]
            y = xd[s, rows, 128:384]
            g1 = lax.dot_general(x, wf[0, s], NT, preferred_element_type=F32)
            u1 = lax.dot_general(x, wf[1, s], NT, preferred_element_type=F32)
            b1 = lax.dot_general(y, wf[2, s], NT, preferred_element_type=F32)
            gate = g1 if gate is None else gate + g1
            up = u1 if up is None else up + u1
            back = b1 if back is None else back + b1
        meta = xd[0, rows, 128:256].astype(F32)
        lane = lax.broadcasted_iota(jnp.int32, (CH, 128), 1)
        whole = pltpu.roll(meta, 124, 1) + pltpu.roll(meta, 120, 1)
        mine = (meta == e.astype(F32)) & (lane >= 52) & (lane < 56)
        w = jnp.sum(jnp.where(mine, whole, 0.0), axis=1, keepdims=True)
        sig = jax.nn.sigmoid(gate)
        act = gate * sig
        prod = act * up
        gh = w * back
        d_gate = gh * up * sig * (1.0 + gate * (1.0 - sig))
        d_up = gh * act
        hb = prod.astype(BF).astype(F32) * back
        hi = hb.astype(BF)
        lo = (hb - hi.astype(F32)).astype(BF)
        row8 = (lax.broadcasted_iota(jnp.int32, (8, 192), 0) == c).astype(F32).astype(BF)
        rp[:, 0:CH] += lax.dot_general(
            row8, hi, NT, preferred_element_type=F32
        ) + lax.dot_general(row8, lo, NT, preferred_element_type=F32)
        dgb, dub = d_gate.astype(BF), d_up.astype(BF)
        dgu_t[c, 0:192, :] = d_gate.T.astype(BF)
        dgu_t[c, 192:384, :] = d_up.T.astype(BF)
        hw_t[c] = (w * prod).T.astype(BF)
        for q in range(4):
            for h in range(2):
                lanes = slice(768 * q + 384 * h, 768 * q + 384 * h + 384)
                p = jnp.dot(dgb, wb[odd, 0, :, lanes], preferred_element_type=F32) + jnp.dot(
                    dub, wb[odd, 1, :, lanes], preferred_element_type=F32
                )
                part[c, q, h] = p.astype(BF)
        for k in range(4):
            rs_copy(c, k).start()

    def stage_f(c):
        odd, a, b = place(c)
        ar, al = (a + 1) % 4, (a + 3) % 4
        rs_copy(c, 0).wait_recv()
        part[c, ar, 0] = (part[c, ar, 0].astype(F32) + fwd[c, 0].astype(F32)).astype(BF)
        rs_copy(c, 4).start()
        rs_copy(c, 1).wait_recv()
        part[c, al, 1] = (part[c, al, 1].astype(F32) + fwd[c, 1].astype(F32)).astype(BF)
        rs_copy(c, 5).start()

    def stage_g(c):
        odd, a, b = place(c)
        at = near.at[c]
        remote(at, at, rs_send.at[c, 0], rs_recv.at[c, 2], peer(me)).wait_recv()
        for h in range(2):
            q = (
                part[c, a, h].astype(F32) + near[c, 0, h].astype(F32) + near[c, 1, h].astype(F32)
            ).astype(BF)
            quart[c, 2 * h] = q[:, 0:256]
            quart[c, 2 * h + 1] = q[:, 128:384]
        rs_copy(c, 6).start()
        rs_copy(c, 7).start()

    def stage_h(c):
        odd, a, b = place(c)
        flip = (c // 2) % 2
        ba = jnp.where(flip == 0, (b + 1) % 4, (b + 3) % 4)
        rs_copy(c, 6).wait_recv()
        quart[c, ba] = (quart[c, ba].astype(F32) + gsum[c].astype(F32)).astype(BF)
        rs_copy(c, 8).start()

    def back_copy(c, k, src, dst, send, recv, split):
        at = src.at[c, k] if split else src.at[c]
        to = ((z + c) % 8) * 2 + k
        return remote(at, dst.at[e], send.at[0], recv.at[c if split else 0], owner(to))

    def send_back(c, src, dst, send, recv, split):
        @pl.when(c > 0)
        def _():
            back_copy(c, 0, src, dst, send, recv, split).start()
            back_copy(c, 1, src, dst, send, recv, split).start()

        @pl.when(c == 0)
        def _():
            back_copy(c, 1 - core, src, dst, send, recv, split).start()
            dst[e] = src[c, core] if split else src[c]

    def back_all(n, dst, send, recv):
        at = dst.at[pl.ds(0, n)]
        return remote(at, at, send.at[0], recv, owner(sib))

    def stage_i(c):
        odd, a, b = place(c)
        at = term.at[c]
        remote(at, at, rs_send.at[c, 1], rs_recv.at[c, 4], peer(me)).wait_recv()
        r = quart[c, b].astype(F32) + term[c, 0].astype(F32) + term[c, 1].astype(F32)
        r = jnp.where(b % 2 == 1, pltpu.roll(r, 192, 1), r)
        pad = jnp.zeros((RET - CAP, 256), F32)
        ret[c, 0] = jnp.concatenate([r[0:CAP], pad], axis=0).astype(BF)
        ret[c, 1] = jnp.concatenate([r[CAP:CH], pad], axis=0).astype(BF)
        send_back(c, ret, got, ret_send, ret_recv, True)

    def choose(first, last):
        def one(j, carry):
            chosen[j] = picks(xin[:, 128:256].astype(F32), j.astype(F32))
            return carry

        lax.fori_loop(first, last, one, 0, unroll=4)

    def stage_j(c):
        @pl.when(c > 0)
        def _():
            back_all(2, got, ret_send, ret_recv.at[c]).wait_recv()

        @pl.when(c == 0)
        def _():
            back_all(1, got, ret_send, ret_recv.at[c]).wait_recv()

        total = gacc[...]
        for k in range(2):
            j = ((z + 8 - c) % 8) * 2 + k
            total = total + jnp.dot(
                chosen[j, :, 0:RET], got[j], preferred_element_type=F32
            )
        gacc[...] = total

    def routes(c):
        meta = xin[:, 128:256].astype(F32)
        total = racc[...]
        for k in range(2):
            j = ((z + 8 - c) % 8) * 2 + k
            r = rgot[j]
            r = jnp.where(core == 1, pltpu.roll(r, 256 - CAP, 1), r)[:, 0:128]
            hi = r.astype(BF).astype(F32)
            row = lax.broadcasted_iota(jnp.int32, (8, 128), 0)
            both = jnp.where(row == 0, hi, jnp.where(row == 1, r - hi, 0.0)).astype(BF)
            value = jnp.sum(
                lax.dot_general(chosen[j], both, NT, preferred_element_type=F32),
                axis=1, keepdims=True,
            )
            total = total + jnp.where((meta == j.astype(F32)) & id_lane, value, 0.0)
        racc[...] = total

    def guard(cond, f, *args):
        @pl.when(cond)
        def _():
            with jax.named_scope(f.__name__):
                f(*args)

    def prepare(k):
        load[k].wait()
        for s in range(NB):
            w = wraw[k % 2, :, SH * s : SH * s + SH]
            at = 0 if k < 2 else 64
            wf[k, s, 0:SH, at : at + SH] = w
            if k < 2:
                t = (s % 4) * 4 + s // 4
                wb[0, k, 0:SH, 192 * s : 192 * s + SH] = w
                wb[1, k, 0:SH, 192 * t : 192 * t + SH] = w
        if k == 0:
            load[2].start()

    def drain_ag(c):
        ag_all(c, 0, 15).wait_send()

    def drain_ag(c):
        ag_all(c, 0, 15).wait_send()

    def drain_rs(c):
        at = part.at[c, pl.ds(0, 3)]
        remote(at, at, rs_send.at[c, 0], rs_recv.at[c, 0], peer(me)).wait_send()
        at = quart.at[c, pl.ds(0, 3)]
        remote(at, at, rs_send.at[c, 1], rs_recv.at[c, 0], peer(me)).wait_send()

    zfirst()
    buf[e] = xin[...]
    stage_x(0)
    stage_a(0)
    rp[...] = jnp.zeros_like(rp)
    gacc[...] = jnp.zeros_like(gacc)
    racc[...] = jnp.zeros_like(racc)
    wf[...] = jnp.zeros_like(wf)
    wb[...] = jnp.zeros_like(wb)
    prepare(0)
    prepare(1)
    zstage(1)
    stage_x(1)
    stage_a(1)
    stage_b(0)
    choose(0, 8)
    zstage(2)
    stage_x(2)
    stage_a(2)
    stage_c(0)
    stage_b(1)
    zstage(3)
    stage_x(3)
    stage_a(3)
    stage_d(0)
    prepare(2)
    choose(8, 16)
    zstage(4)
    stage_c(1)

    def step(t, carry):
        guard((t >= 3) & (t < NC - 1), stage_x, t + 1)
        guard((t >= 3) & (t < NC - 1), stage_a, t + 1)
        guard(t >= 2, stage_b, t)
        guard(t >= 2, stage_d, t - 1)
        guard(t >= 3, stage_f, t - 3)
        guard(t >= 2, stage_e, t - 2)
        guard(t >= 2, stage_c, t)
        guard(t >= 3, stage_g, t - 3)
        guard(t >= 4, stage_h, t - 4)
        guard(t >= 5, stage_i, t - 5)
        guard(t >= 6, stage_j, t - 6)
        guard(t >= 4, drain_ag, t - 4)
        guard(t >= 6, drain_rs, t - 6)
        return carry

    lax.fori_loop(2, NC, step, 0)

    def rt(d):
        j = (me + d) % NB
        return remote(rp, rp_all.at[me], rt_send.at[0], rt_recv.at[0], peer(j))

    def rt_all():
        at = rp_all.at[pl.ds(0, NB - 1)]
        return remote(at, at, rt_send.at[0], rt_recv.at[0], peer(me))

    def routes_out():
        for d in range(1, NB):
            rt(d).start()
        rp_all[me] = rp[...]

    def routes_back():
        rt_all().wait_recv()
        total = rp_all[0]
        for j in range(1, NB):
            total = total + rp_all[j]
        for k in range(NC):
            rsend[k] = jnp.broadcast_to(total[k : k + 1, :], (8, 256))
            send_back(k, rsend, rgot, rr_send, rr_recv, False)

    def weight_grads(s):
        gu = hd = None
        for c in range(NC):
            x = xd[s, CH * c : CH * c + CH, 0:256]
            y = xd[s, CH * c : CH * c + CH, 128:384]
            g1 = jnp.dot(dgu_t[c], x, preferred_element_type=F32)
            h1 = jnp.dot(hw_t[c], y, preferred_element_type=F32)
            gu = g1 if gu is None else gu + g1
            hd = h1 if hd is None else hd + h1
        lanes = slice(SH * s, SH * s + SH)
        grads[0, :, lanes] = gu[0:SH, 0:SH]
        grads[1, :, lanes] = gu[192 : 192 + SH, 0:SH]
        grads[2, :, lanes] = hd[0:SH, 64 : 64 + SH]

    def grad_copy(k, i):
        lanes = slice((0, 1152, 1920)[i], (1152, 1920, 2880)[i])
        out = (gg_ref, gu_ref, gd_ref)[k]
        return pltpu.make_async_copy(grads.at[k, :, lanes], out.at[:, 0, lanes], g_sem.at[k])

    def wg(first, last):
        with jax.named_scope("wg"):
            for s in range(first, last):
                weight_grads(s)

    def tail(f, c):
        with jax.named_scope(f.__name__):
            f(c)

    def grads_out(i):
        for k in range(3):
            grad_copy(k, i).start()

    tail(stage_d, 7)
    tail(stage_f, 5)
    tail(stage_e, 6)
    tail(stage_g, 5)
    tail(stage_h, 4)
    tail(stage_i, 3)
    tail(stage_j, 2)
    tail(stage_e, 7)
    routes_out()
    tail(stage_f, 6)
    drain_ag(4)
    wg(0, 4)
    tail(stage_f, 7)
    tail(stage_h, 5)
    tail(stage_i, 4)
    tail(stage_j, 3)
    wg(4, 8)
    tail(stage_g, 6)
    wg(8, 9)
    grads_out(0)
    tail(stage_g, 7)
    tail(stage_i, 5)
    routes_back()
    wg(9, 11)
    grads_out(1)
    tail(stage_h, 6)
    tail(stage_j, 4)
    tail(stage_h, 7)
    wg(11, 14)
    tail(stage_i, 6)
    tail(stage_i, 7)
    tail(stage_j, 5)
    wg(14, 16)
    grads_out(2)
    tail(stage_j, 6)
    back_all(NB - 1, rgot, rr_send, rr_recv.at[0]).wait_recv()
    for k in range(NC):
        tail(routes, k)
    gr_ref[...] = racc[...].T[52:56]
    with jax.named_scope("drain"):
        for k in range(5, NC):
            drain_ag(k)
        for k in range(2, NC):
            drain_rs(k)
        rt_all().wait_send()
        at = buf.at[pl.ds(0, 15)]
        remote(at, at, z_send.at[0], z_recv.at[0, 0], owner(sib)).wait_send()
        back_all(NB - 1, rgot, rr_send, rr_recv.at[0]).wait_send()
    with jax.named_scope("grads"):
        for k in range(3):
            out = (gg_ref, gu_ref, gd_ref)[k]
            pltpu.make_async_copy(grads.at[k], out.at[:, 0], g_sem.at[k]).wait()
    tail(stage_j, 7)
    back_all(NB - 1, got, ret_send, ret_recv.at[0]).wait_send()
    with jax.named_scope("gin"):
        gin_ref[...] = gacc[...].T[0:SH].astype(BF)


def layer(x, dy, ids, rw, w_gate, w_up, w_down):
    vm = pl.BlockSpec(memory_space=pltpu.VMEM)
    hbm = pl.BlockSpec(memory_space=pl.ANY)
    grad = jax.ShapeDtypeStruct((SH, 1, NB * SH), F32)
    dma = pltpu.SemaphoreType.DMA
    return pl.pallas_call(
        layer_kernel,
        out_shape=[
            grad, grad, grad,
            jax.ShapeDtypeStruct((SH, TOK), BF),
            jax.ShapeDtypeStruct((4, TOK), F32),
        ],
        in_specs=[vm] * 4 + [hbm] * 3,
        out_specs=[hbm] * 3 + [vm] * 2,
        scratch_shapes=[
            pltpu.VMEM((TOK, W2), BF),
            pltpu.VMEM((NB, TOK, W2), BF),
            pltpu.VMEM((NB, ROWS, W2), BF),
            pltpu.VMEM((2, SH, NB * SH), BF),
            pltpu.VMEM((3, NB, 192, 256), BF),
            pltpu.VMEM((2, 2, 192, NB * 192), BF),
            pltpu.VMEM((NC, 4, 2, CH, 384), BF),
            pltpu.VMEM((NC, 2, CH, 384), BF),
            pltpu.VMEM((NC, 2, 2, CH, 384), BF),
            pltpu.VMEM((NC, 4, CH, 256), BF),
            pltpu.VMEM((NC, CH, 256), BF),
            pltpu.VMEM((NC, 2, CH, 256), BF),
            pltpu.VMEM((NC, 384, CH), BF),
            pltpu.VMEM((NC, 192, CH), BF),
            pltpu.VMEM((8, 256), F32),
            pltpu.VMEM((NB, 8, 256), F32),
            pltpu.VMEM((NC, 2, RET, 256), BF),
            pltpu.VMEM((NB, RET, 256), BF),
            pltpu.VMEM((NC, 8, 256), F32),
            pltpu.VMEM((NB, 8, 256), F32),
            pltpu.VMEM((TOK, 256), F32),
            pltpu.VMEM((TOK, 128), F32),
            pltpu.VMEM((3, SH, NB * SH), F32),
            pltpu.VMEM((NB, TOK, 128), BF),
            dma((3,)),
            dma((1,)),
            dma((4, 2)),
            dma((8,)),
            dma((NC,)),
            dma((NC, 4)),
            dma((NC, 2)),
            dma((NC, 5)),
            dma((1,)),
            dma((1,)),
            dma((1,)),
            dma((NC,)),
            dma((1,)),
            dma((1,)),
            dma((3,)),
        ],
        compiler_params=pltpu.CompilerParams(
            collective_id=0, has_side_effects=True, vmem_limit_bytes=67043328
        ),
        name="layer",
    )(x, dy, ids, rw, w_gate, w_up, w_down)


def finish_kernel(g0, g1, g2, gin_ref, gr_ref, o0, o1, o2, ogin_ref, ogr_ref, held, sem):
    def piece(k, out):
        outer = ((o0, o1, o2) if out else (g0, g1, g2))[k]
        src, dst = (held.at[k], outer) if out else (outer, held.at[k])
        return pltpu.make_async_copy(src, dst, sem.at[out, k])

    for k in range(3):
        piece(k, 0).start()
    ogin_ref[...] = gin_ref[...]
    ogr_ref[...] = gr_ref[...]
    for k in range(3):
        piece(k, 0).wait()
        piece(k, 1).start()
    for k in range(3):
        piece(k, 1).wait()


def finish(*arrays):
    vm = pl.BlockSpec(memory_space=pltpu.VMEM)
    hbm = pl.BlockSpec(memory_space=pl.ANY)
    return pl.pallas_call(
        finish_kernel,
        out_shape=[jax.ShapeDtypeStruct(a.shape, a.dtype) for a in arrays],
        in_specs=[hbm] * 3 + [vm] * 2,
        out_specs=[hbm] * 3 + [vm] * 2,
        scratch_shapes=[
            pltpu.VMEM((3, SH, 1, NB * SH), F32),
            pltpu.SemaphoreType.DMA((2, 3)),
        ],
        name="finish",
    )(*arrays)


def per_device(inputs, out_grad, expert_ids, route_weight, w_gate, w_up, w_down):
    found = layer(
        inputs.T, out_grad.T, expert_ids.T, route_weight.T, w_gate[0], w_up[0], w_down[0]
    )
    gg, gu, gd, grad_input, grad_route = finish(*found)
    grads = [jnp.transpose(g, (1, 0, 2)) for g in (gg, gu, gd)]
    return (grad_input.T, grad_route.T, *grads)


def solution(mesh):
    torus = Mesh(
        mesh.devices.reshape(mesh.shape["expert"], 4, 4), ("expert", "hidden_0", "hidden_1")
    )
    placed = (
        P("expert", HIDDEN),
        P("expert", HIDDEN),
        P("expert", None),
        P("expert", None),
        P("expert", HIDDEN, None),
        P("expert", HIDDEN, None),
        P("expert", HIDDEN, None),
    )
    return jax.shard_map(
        per_device,
        mesh=torus,
        in_specs=placed,
        out_specs=(
            P("expert", HIDDEN),
            P("expert", None),
            P("expert", HIDDEN, None),
            P("expert", HIDDEN, None),
            P("expert", HIDDEN, None),
        ),
        check_vma=False,
    )
```
